512 devices in a mesh: va: 16 (over z_hi, y), vb: 8 (over z_lo, core), occ: 4 (over x).
Axes of the slice: x: 4, y: 8, z: 8 (z_hi: 2, z_lo: 4; z = z_hi * 4 + z_lo), core: 2. Of those that a mesh axis runs over, the one named last changes fastest.
Arguments:
- amplitudes: bfloat16 [6, 1536, 1536], P(None, 'va', 'occ'), may hold values from -6 to 6
- bra_factor: bfloat16 [16, 1536, 1536], P('vb', 'va'), may hold values from -0.078125 to 0.078125
- ket_factor: bfloat16 [16, 1536, 1536], P('va', ('vb', 'occ')), may hold values from -0.15625 to 0.15625
- pair_list: int32 [8, 4], replicated, may hold values from 0 to 5, as said below
Outputs:
- ladder: float32 [6, 1536, 1536], P(None, 'va', ('vb', 'occ'))
The draws below stay inside these ranges and needn't reach their ends.
Inputs may be any that keep to these rules, and one draw needn't show every extreme that they name: `pair_list`: each row names 4 different pairs, and every pair of 0 to 5 is named by some row.
All inputs are finite; a program needn't handle non-finite values.
Results may differ from the reference program's by a relative error of at most 0.0042.
Values may be sent and summed in bfloat16 or wider, within the bound.
No kernel may reach another device: no remote copies, remote signals or barrier semaphores. Data moves between devices by JAX's collectives and lax.ppermute only.
A program may use at most 64 MiB of HBM per device.

```python
import jax
import jax.numpy as jnp

NV = 1536
QC = 1
SPANS = 2
PAIRS = 6
PICK = 4
NQW = 16
N_VB = 8


def draw_pair_list(key, part):
    order = jax.random.permutation(jax.random.fold_in(key, 17), PAIRS)
    places = (jnp.arange(N_VB, dtype=jnp.int32)[:, None] * PICK + jnp.arange(PICK, dtype=jnp.int32)[None, :]) % PAIRS
    return order[places].astype(jnp.int32)


def spiked(array, key, source, target, parts, factor):
    def block_of(position):
        return (jnp.arange(array.shape[position]) // (array.shape[position] // parts)).reshape((-1,) + (1,) * (array.ndim - 1 - position))

    first = jax.random.permutation(key, parts)[block_of(target)]
    second = (block_of(target) + parts // 2) % parts
    return jnp.where((block_of(source) == first) | (block_of(source) == second), factor * array, array)


def level_of(own_key, dims, cuts, low, largest):
    factor_of, own = 1.0, jax.random.fold_in(own_key, 6)
    for dim, parts in cuts:
        draws = jnp.exp(jax.random.uniform(jax.random.fold_in(own, dim), (parts,), jnp.float32, low / len(cuts), largest / len(cuts)))
        factor_of = factor_of * jnp.repeat(draws, dims[dim] // parts).reshape([-1 if axis == dim else 1 for axis in range(len(dims))])
    return factor_of


def normal_values(own_key, shape, scale, most, split=(), kind=jnp.bfloat16):
    factor_of = level_of(own_key, shape, split, -0.22, 0.18) if split else 1.0
    drawn = jax.random.normal(own_key, shape, jnp.float32) * scale * factor_of
    return jnp.minimum(jnp.maximum(drawn, -most), most).astype(kind)


def gaussian_with(rng, shape, scale, reach, shards, heavy, kind=jnp.bfloat16):
    entries = scale * jax.random.normal(rng, shape, jnp.float32)
    if shards:
        entries = entries * level_of(rng, shape, shards, -0.22, 0.18)
    return jnp.clip(spiked(entries, jax.random.fold_in(rng, 3), *heavy), -reach, reach).astype(kind)


def setup_inputs(seed: int = 0) -> dict:
    key_list = jax.random.split(jax.random.key(seed), 5)
    return {
        "amplitudes": normal_values(key_list[0], (PAIRS, NV, NV), 1.0, 6.0, ((1, 16), (2, 4))),
        "bra_factor": gaussian_with(key_list[1], (NQW, NV, NV), (NV * QC * SPANS * N_VB // 2) ** -0.5, 0.078125, ((0, 8), (1, 16)), (1, 2, 16, 2.0)),
        "ket_factor": normal_values(key_list[2], (NQW, NV, NV), NV ** -0.5, 0.15625, ((0, 16), (1, 32))),
        "pair_list": draw_pair_list(jax.random.fold_in(key_list[4], 71), 0),
    }


def reference(amplitudes, bra_factor, ket_factor, pair_list):
    group = QC * SPANS
    ladder = jnp.zeros((PAIRS, NV, NV), jnp.float32)
    for step in range(N_VB):
        picks = pair_list[step]
        ket_group = ket_factor[step * group:(step + 1) * group].astype(jnp.float32)
        bra_group = bra_factor[step * group:(step + 1) * group].astype(jnp.float32)
        chosen = jnp.take(amplitudes, picks, axis=0).astype(jnp.float32)
        half = jnp.einsum('qbd,kcd->qkcb', ket_group, chosen).astype(jnp.bfloat16)
        partial_terms = jnp.einsum('qca,qkcb->kab', bra_group, half.astype(jnp.float32))
        ladder = ladder.at[picks].add(partial_terms)
    return ladder
```

```python
import jax
import jax.numpy as jnp
from jax import lax
from jax.experimental import pallas as pl
from jax.experimental.pallas import tpu as pltpu
from jax.sharding import Mesh
from jax.sharding import PartitionSpec as P

AXES = ("zh", "y", "zl", "core", "x")
VA = ("zh", "y")
F32 = jnp.float32
BF16 = jnp.bfloat16
VMEM = pl.BlockSpec(memory_space=pltpu.VMEM)
SMEM = pl.BlockSpec(memory_space=pltpu.SMEM)
PARAMS = pltpu.CompilerParams(vmem_limit_bytes=20 << 20)


def shifted(block, axis, by):
    n = lax.axis_size(axis)
    return lax.ppermute(block, axis, [(i, (i + by) % n) for i in range(n)])


def copies_from(array, axis):
    copies = jnp.broadcast_to(array, (lax.axis_size(axis), *array.shape))
    return lax.all_to_all(copies, axis, 0, 0, tiled=True)


def half_kernel(lists, where, ket, mine, theirs, half):
    zh, zl, core = where[0], where[1], where[2]
    cols = ket.shape[1]
    parts, own, rows, width = mine.shape
    n_q = ket.shape[0]
    places = []
    for other in range(2):
        side = core if other == 0 else 1 - core
        for s in range(4):
            for j in range(2):
                places.append(4 * ((zl - s + 4) % 4) + 2 * side + j)
    lhs = []
    for q in places:
        high = q // 8
        lhs.append(ket[(q % 8) * 2 + jnp.where(high == zh, 0, 1)])
    lhs = jnp.concatenate(lhs, axis=0)
    out = None
    for x in range(parts):
        rhs = jnp.concatenate([mine[x], theirs[x]], axis=0).reshape(2 * own * rows, width)
        term = lax.dot_general(
            lhs[:, x * width : (x + 1) * width], rhs, (((1,), (1,)), ((), ())), preferred_element_type=F32
        )
        out = term if out is None else out + term
    for side in range(2):
        first = own * (core if side == 0 else 1 - core)
        for k in range(own):
            p = first + k
            at = side * own + k
            for i in range(n_q):
                group = places[i] // 2
                wanted = lists[group, 0] == p
                for m in range(1, lists.shape[1]):
                    wanted = jnp.logical_or(wanted, lists[group, m] == p)
                block = out[i * cols : (i + 1) * cols, at * rows : (at + 1) * rows]
                block = jnp.where(wanted, block, 0.0).astype(BF16)
                half[pl.ds(pl.multiple_of(p * cols, 16), cols), i * rows : (i + 1) * rows] = block


def total_kernel(half, *refs):
    bras, out = refs[:-1], refs[-1]
    rows = bras[0].shape[1]
    n_a = bras[0].shape[2]
    m = half.shape[0]
    width = 4 * rows
    keep = m * rows // 128
    lhs = half[...]
    for j in range(0, n_a, width):
        rhs = jnp.concatenate([b[i, :, j : j + width] for b in bras for i in range(b.shape[0])], axis=0)
        sums = jnp.dot(lhs, rhs, preferred_element_type=F32)
        for i in range(4):
            block = sums[:, i * rows : (i + 1) * rows]
            tail = jnp.concatenate([block[keep:, 32 * s : 32 * s + 32] for s in range(rows // 32)], axis=0)
            out[j // rows + i] = jnp.concatenate([block[:keep], tail], axis=1).astype(BF16)


def sum_kernel(parts, out):
    rows = out.shape[1]
    keep, step = parts.shape[1], out.shape[0] - parts.shape[1]
    sums = parts[0].astype(F32)
    for i in range(1, parts.shape[0]):
        sums = sums + parts[i].astype(F32)
    out[:keep, :] = sums[:, :rows]
    tail = [sums[step * s : step * (s + 1), rows:] for s in range(rows // 32)]
    out[keep:, :] = jnp.concatenate(tail, axis=1)


def per_device(amplitudes, bra_factor, ket_factor, pair_list):
    pairs, rows, width = amplitudes.shape
    cols = ket_factor.shape[1]
    n_a = bra_factor.shape[2]
    core = lax.axis_index("core")
    where = jnp.stack([lax.axis_index("zh"), lax.axis_index("zl"), core]).astype(jnp.int32)

    ket = jnp.concatenate([ket_factor, shifted(ket_factor, "zh", 1)], axis=0)
    ket = lax.all_gather(ket, "y", axis=0, tiled=True)
    bras = [bra_factor] + [shifted(bra_factor, "zl", s) for s in range(1, 4)]
    bras = bras + [shifted(b, "core", 1) for b in bras]
    mine = copies_from(lax.dynamic_slice_in_dim(amplitudes, core * (pairs // 2), pairs // 2, 0), "x")
    theirs = shifted(mine, "core", 1)

    n_q = 2 * len(bras)
    half = pl.pallas_call(
        half_kernel,
        in_specs=[SMEM, SMEM, VMEM, VMEM, VMEM],
        out_specs=VMEM,
        out_shape=jax.ShapeDtypeStruct((pairs * cols, n_q * rows), BF16),
        compiler_params=PARAMS,
        name="half",
    )(pair_list, where, ket, mine, theirs)
    n_va = n_a // rows
    total = pl.pallas_call(
        total_kernel,
        in_specs=[VMEM] * (1 + len(bras)),
        out_specs=VMEM,
        out_shape=jax.ShapeDtypeStruct((n_va, pairs * cols * rows // 128, 128), BF16),
        compiler_params=PARAMS,
        name="total",
    )(half, *bras)
    total = lax.all_to_all(total, VA, 0, 0, tiled=True)
    out = pl.pallas_call(
        sum_kernel,
        in_specs=[VMEM],
        out_specs=VMEM,
        out_shape=jax.ShapeDtypeStruct((pairs * cols, rows), F32),
        compiler_params=PARAMS,
        name="sum",
    )(total)
    return out.reshape(pairs, cols, rows).transpose(0, 2, 1)


def solution(mesh):
    torus = Mesh(mesh.devices.reshape(2, 8, 4, 2, 4), AXES)
    return jax.shard_map(
        per_device,
        mesh=torus,
        in_specs=(P(None, VA, "x"), P(("zl", "core"), VA, None), P(VA, ("zl", "core", "x"), None), P()),
        out_specs=P(None, VA, ("zl", "core", "x")),
        check_vma=False,
    )
```

```python
import jax
import jax.numpy as jnp
from jax import lax
from jax.experimental import pallas as pl
from jax.experimental.pallas import tpu as pltpu
from jax.sharding import Mesh
from jax.sharding import PartitionSpec as P

AXES = ("zh", "y4", "y0", "zl", "core", "x")
VA = ("zh", "y4", "y0")
F32 = jnp.float32
BF16 = jnp.bfloat16
VMEM = pl.BlockSpec(memory_space=pltpu.VMEM)
SMEM = pl.BlockSpec(memory_space=pltpu.SMEM)
PARAMS = pltpu.CompilerParams(vmem_limit_bytes=20 << 20)
DIRECT = 512


def shifted(block, axis, by):
    n = lax.axis_size(axis)
    return lax.ppermute(block, axis, [(i, (i + by) % n) for i in range(n)])


def copies_from(array, axis):
    copies = jnp.broadcast_to(array, (lax.axis_size(axis), *array.shape))
    return lax.all_to_all(copies, axis, 0, 0, tiled=True)


def half_kernel(lists, where, *refs):
    kets, (mine, theirs, half, ket) = refs[:4], refs[4:]
    zh, y4, y0, _, core, x = [where[i] for i in range(6)]
    _, cols, _ = kets[0].shape
    parts, blocks, own, rows, width = mine.shape
    for s in range(4):
        for h in range(2):
            ket[2 * s + h] = kets[s][h]
    places, groups = [], []
    for r in range(2):
        side = core if r == 0 else 1 - core
        for z in range(4):
            q = 4 * z + 2 * side + y0
            high = q // 8
            s = (y4 - (q % 8) // 2 + 4) % 4
            places.append(2 * s + jnp.where(high == zh, 0, 1))
            groups.append(q // 2)
    n_q = len(places)
    out = None
    for s in range(parts):
        at = pl.multiple_of(((x - s + 4) % 4) * width, 128)
        lhs = jnp.concatenate([ket[q, :, pl.ds(at, width)] for q in places], axis=0)
        rhs = jnp.concatenate([mine[s], theirs[s]], axis=0).reshape(2 * blocks * own * rows, width)
        term = lax.dot_general(lhs, rhs, (((1,), (1,)), ((), ())), preferred_element_type=F32)
        out = term if out is None else out + term
    for side in range(2):
        first = own * (core if side == 0 else 1 - core)
        for k in range(own):
            p = first + k
            for i in range(n_q):
                wanted = lists[groups[i], 0] == p
                for m in range(1, lists.shape[1]):
                    wanted = jnp.logical_or(wanted, lists[groups[i], m] == p)
                for b in range(blocks):
                    at = ((side * blocks + b) * own + k) * rows
                    block = out[i * cols : (i + 1) * cols, at : at + rows]
                    block = jnp.where(wanted, block, 0.0).astype(BF16)
                    to = (i * blocks + b) * rows
                    half[pl.ds(pl.multiple_of(p * cols, 16), cols), to : to + rows] = block


def total_kernel(where, half, direct, direct_other, shared, shared_other, out):
    zl = where[3]
    rows = direct.shape[2]
    n_direct, n_shared = direct.shape[3], shared.shape[4]
    n_a = n_direct + shared.shape[0] * n_shared
    m = half.shape[0]
    width = 4 * rows
    keep = m * rows // 128
    lhs = half[...]

    def column(side, z, b, start):
        ref = (direct, direct_other)[side] if start < n_direct else (shared, shared_other)[side]
        if start < n_direct:
            return ref[(zl - z + 4) % 4, b, :, start : start + 128]
        x, at = divmod(start - n_direct, n_shared)
        return ref[x, z, b, :, at : at + 128]

    for j in range(0, n_a, width):
        rhs = jnp.concatenate(
            [
                jnp.concatenate([column(side, z, b, t) for t in range(j, j + width, 128)], axis=1)
                for side in range(2)
                for z in range(4)
                for b in range(2)
            ],
            axis=0,
        )
        sums = jnp.dot(lhs, rhs, preferred_element_type=F32)
        for i in range(4):
            block = sums[:, i * rows : (i + 1) * rows]
            tail = jnp.concatenate([block[keep:, 32 * s : 32 * s + 32] for s in range(rows // 32)], axis=0)
            out[j // rows + i] = jnp.concatenate([block[:keep], tail], axis=1).astype(BF16)


def sum_kernel(parts, out):
    rows = out.shape[1]
    keep, step = parts.shape[1], out.shape[0] - parts.shape[1]
    sums = parts[0].astype(F32)
    for i in range(1, parts.shape[0]):
        sums = sums + parts[i].astype(F32)
    out[:keep, :] = sums[:, :rows]
    tail = [sums[step * s : step * (s + 1), rows:] for s in range(rows // 32)]
    out[keep:, :] = jnp.concatenate(tail, axis=1)


def per_device(amplitudes, bra_factor, ket_factor, pair_list):
    pairs, rows, _ = amplitudes.shape
    cols = ket_factor.shape[1]
    n_a = bra_factor.shape[2]
    core = lax.axis_index("core")
    y0 = lax.axis_index("y0")
    x = lax.axis_index("x")
    where = jnp.stack([lax.axis_index(name) for name in AXES]).astype(jnp.int32)
    n_shared = (n_a - DIRECT) // 4

    ket_other = shifted(ket_factor, "zh", 1)

    def bra_of(parity):
        straight = lax.dynamic_slice(bra_factor, (parity, 0, 0), (1, rows, DIRECT))
        quarter = lax.dynamic_slice(bra_factor, (parity, 0, DIRECT + n_shared * x), (1, rows, n_shared))
        return jnp.concatenate([straight, quarter], axis=2)

    bra = jnp.concatenate([bra_of(y0), shifted(bra_of(1 - y0), "y0", 1)], axis=0)
    tau = lax.dynamic_slice_in_dim(amplitudes, core * (pairs // 2), pairs // 2, 0)
    tau = jnp.stack([tau, shifted(tau, "y0", 1)])
    shared = copies_from(bra[:, :, DIRECT:], "zl")
    shared = copies_from(shared, "x")
    mine = jnp.stack([tau] + [shifted(tau, "x", s) for s in range(1, 4)])
    ket = jnp.concatenate([ket_factor, ket_other], axis=0)
    kets = [ket] + [shifted(ket, "y4", s) for s in range(1, 4)]
    direct = bra[:, :, :DIRECT]
    direct = jnp.stack([direct] + [shifted(direct, "zl", s) for s in range(1, 4)])
    theirs = shifted(mine, "core", 1)
    direct_other = shifted(direct, "core", 1)
    shared_other = shifted(shared, "core", 1)

    n_q = 8
    half = pl.pallas_call(
        half_kernel,
        in_specs=[SMEM, SMEM] + [VMEM] * 6,
        out_specs=VMEM,
        out_shape=jax.ShapeDtypeStruct((pairs * cols, n_q * 2 * rows), BF16),
        scratch_shapes=[pltpu.VMEM((n_q, cols, ket.shape[2]), BF16)],
        compiler_params=PARAMS,
        name="half",
    )(pair_list, where, *kets, mine, theirs)
    n_va = n_a // rows
    total = pl.pallas_call(
        total_kernel,
        in_specs=[SMEM] + [VMEM] * 5,
        out_specs=VMEM,
        out_shape=jax.ShapeDtypeStruct((n_va, pairs * cols * rows // 128, 128), BF16),
        compiler_params=PARAMS,
        name="total",
    )(where, half, direct, direct_other, shared, shared_other)
    total = lax.all_to_all(total, VA, 0, 0, tiled=True)
    out = pl.pallas_call(
        sum_kernel,
        in_specs=[VMEM],
        out_specs=VMEM,
        out_shape=jax.ShapeDtypeStruct((pairs * cols, rows), F32),
        compiler_params=PARAMS,
        name="sum",
    )(total)
    return out.reshape(pairs, cols, rows).transpose(0, 2, 1)


def solution(mesh):
    torus = Mesh(mesh.devices.reshape(2, 4, 2, 4, 2, 4), AXES)
    return jax.shard_map(
        per_device,
        mesh=torus,
        in_specs=(P(None, VA, "x"), P(("zl", "core"), VA, None), P(VA, ("zl", "core", "x"), None), P()),
        out_specs=P(None, VA, ("zl", "core", "x")),
        check_vma=False,
    )
```

```python
import jax
import jax.numpy as jnp
from jax import lax
from jax.experimental import pallas as pl
from jax.experimental.pallas import tpu as pltpu
from jax.sharding import Mesh
from jax.sharding import PartitionSpec as P

AXES = ("zh", "y", "zl", "core", "x")
VA = ("zh", "y")
F32 = jnp.float32
BF16 = jnp.bfloat16
VMEM = pl.BlockSpec(memory_space=pltpu.VMEM)
SMEM = pl.BlockSpec(memory_space=pltpu.SMEM)
PARAMS = pltpu.CompilerParams(vmem_limit_bytes=20 << 20)


def shifted(block, axis, by):
    n = lax.axis_size(axis)
    return lax.ppermute(block, axis, [(i, (i + by) % n) for i in range(n)])


def copies_from(array, axis):
    copies = jnp.broadcast_to(array, (lax.axis_size(axis), *array.shape))
    return lax.all_to_all(copies, axis, 0, 0, tiled=True)


def half_kernel(lists, where, *refs):
    kets, (mine, theirs, half, ket) = refs[:8], refs[8:]
    zh, y, _, core, x = [where[i] for i in range(5)]
    cols = ket.shape[1]
    parts, own, rows, width = mine.shape
    for d in range(8):
        for h in range(2):
            ket[2 * d + h] = kets[d][h]
    places, groups = [], []
    for r in range(2):
        side = core if r == 0 else 1 - core
        for z in range(4):
            for j in range(2):
                q = 4 * z + 2 * side + j
                high = q // 8
                places.append(2 * ((y - q % 8 + 8) % 8) + jnp.where(high == zh, 0, 1))
                groups.append(2 * z + side)
    n_q = len(places)
    out = None
    for s in range(parts):
        at = pl.multiple_of(((x - s + 4) % 4) * width, 128)
        lhs = jnp.concatenate([ket[q, :, pl.ds(at, width)] for q in places], axis=0)
        rhs = jnp.concatenate([mine[s], theirs[s]], axis=0).reshape(2 * own * rows, width)
        term = lax.dot_general(lhs, rhs, (((1,), (1,)), ((), ())), preferred_element_type=F32)
        out = term if out is None else out + term
    for side in range(2):
        first = own * (core if side == 0 else 1 - core)
        for k in range(own):
            p = first + k
            at = (side * own + k) * rows
            for i in range(n_q):
                wanted = lists[groups[i], 0] == p
                for m in range(1, lists.shape[1]):
                    wanted = jnp.logical_or(wanted, lists[groups[i], m] == p)
                block = out[i * cols : (i + 1) * cols, at : at + rows]
                block = jnp.where(wanted, block, 0.0).astype(BF16)
                half[pl.ds(pl.multiple_of(p * cols, 16), cols), i * rows : (i + 1) * rows] = block


def total_kernel(half, mine, theirs, out):
    parts, places, blocks, rows, width = mine.shape
    m = half.shape[0]
    keep = m * rows // 128
    lhs = half[...]
    for x in range(parts):
        rhs = jnp.concatenate([ref[x].reshape(places * blocks * rows, width) for ref in (mine, theirs)], axis=0)
        sums = jnp.dot(lhs, rhs, preferred_element_type=F32)
        for i in range(width // rows):
            block = sums[:, i * rows : (i + 1) * rows]
            tail = jnp.concatenate([block[keep:, 32 * s : 32 * s + 32] for s in range(rows // 32)], axis=0)
            out[x * (width // rows) + i] = jnp.concatenate([block[:keep], tail], axis=1).astype(BF16)


def sum_kernel(parts, out):
    rows = out.shape[1]
    keep, step = parts.shape[1], out.shape[0] - parts.shape[1]
    sums = parts[0].astype(F32)
    for i in range(1, parts.shape[0]):
        sums = sums + parts[i].astype(F32)
    out[:keep, :] = sums[:, :rows]
    tail = [sums[step * s : step * (s + 1), rows:] for s in range(rows // 32)]
    out[keep:, :] = jnp.concatenate(tail, axis=1)


def per_device(amplitudes, bra_factor, ket_factor, pair_list):
    pairs, rows, _ = amplitudes.shape
    cols = ket_factor.shape[1]
    n_a = bra_factor.shape[2]
    core = lax.axis_index("core")
    where = jnp.stack([lax.axis_index(name) for name in AXES]).astype(jnp.int32)
    n_own = n_a // lax.axis_size("x")

    ket = jnp.concatenate([ket_factor, shifted(ket_factor, "zh", 1)], axis=0)
    ahead, behind = [ket], [ket]
    for s in range(1, 5):
        ahead.append(shifted(ahead[-1], "y", 1))
        if s < 4:
            behind.append(shifted(behind[-1], "y", -1))
    kets = ahead + behind[:0:-1]
    own = lax.dynamic_slice_in_dim(bra_factor, n_own * lax.axis_index("x"), n_own, 2)
    bra = copies_from(copies_from(own, "zl"), "x")
    tau = lax.dynamic_slice_in_dim(amplitudes, core * (pairs // 2), pairs // 2, 0)
    mine = jnp.stack([tau] + [shifted(tau, "x", s) for s in range(1, 4)])
    theirs = shifted(mine, "core", 1)
    bra_other = shifted(bra, "core", 1)

    n_q = 2 * bra.shape[1] * bra.shape[2]
    half = pl.pallas_call(
        half_kernel,
        in_specs=[SMEM, SMEM] + [VMEM] * (len(kets) + 2),
        out_specs=VMEM,
        out_shape=jax.ShapeDtypeStruct((pairs * cols, n_q * rows), BF16),
        scratch_shapes=[pltpu.VMEM((n_q, cols, ket.shape[2]), BF16)],
        compiler_params=PARAMS,
        name="half",
    )(pair_list, where, *kets, mine, theirs)
    n_va = n_a // rows
    total = pl.pallas_call(
        total_kernel,
        in_specs=[VMEM] * 3,
        out_specs=VMEM,
        out_shape=jax.ShapeDtypeStruct((n_va, pairs * cols * rows // 128, 128), BF16),
        compiler_params=PARAMS,
        name="total",
    )(half, bra, bra_other)
    total = lax.all_to_all(total, VA, 0, 0, tiled=True)
    out = pl.pallas_call(
        sum_kernel,
        in_specs=[VMEM],
        out_specs=VMEM,
        out_shape=jax.ShapeDtypeStruct((pairs * cols, rows), F32),
        compiler_params=PARAMS,
        name="sum",
    )(total)
    return out.reshape(pairs, cols, rows).transpose(0, 2, 1)


def solution(mesh):
    torus = Mesh(mesh.devices.reshape(2, 8, 4, 2, 4), AXES)
    return jax.shard_map(
        per_device,
        mesh=torus,
        in_specs=(P(None, VA, "x"), P(("zl", "core"), VA, None), P(VA, ("zl", "core", "x"), None), P()),
        out_specs=P(None, VA, ("zl", "core", "x")),
        check_vma=False,
    )
```

```python
import jax
import jax.numpy as jnp
from jax import lax
from jax.experimental import pallas as pl
from jax.experimental.pallas import tpu as pltpu
from jax.sharding import Mesh
from jax.sharding import PartitionSpec as P

AXES = ("zh", "y", "zl", "core", "x")
VA = ("zh", "y")
F32 = jnp.float32
BF16 = jnp.bfloat16
VMEM = pl.BlockSpec(memory_space=pltpu.VMEM)
SMEM = pl.BlockSpec(memory_space=pltpu.SMEM)
PARAMS = pltpu.CompilerParams(vmem_limit_bytes=16 << 20)


def shifted(block, axis, by):
    n = lax.axis_size(axis)
    return lax.ppermute(block, axis, [(i, (i + by) % n) for i in range(n)])


def both_ways(block):
    n = lax.axis_size("x")
    route = [(n * c + i, n * c + (i + 1 - 2 * c) % n) for i in range(n) for c in range(2)]
    return lax.ppermute(block, ("core", "x"), route)


def copies_from(array, axis):
    copies = jnp.broadcast_to(array, (lax.axis_size(axis), *array.shape))
    return lax.all_to_all(copies, axis, 0, 0, tiled=True)


def half_kernel(lists, where, *refs):
    kets, (own, near, near_other, far, far_other, half, ket) = refs[:8], refs[8:]
    zh, y, _, core, x = [where[i] for i in range(5)]
    cols = ket.shape[1]
    n_own, rows, width = far.shape
    for d in range(8):
        for h in range(2):
            ket[2 * d + h] = kets[d][h]
    places, groups = [], []
    for r in range(2):
        side = core if r == 0 else 1 - core
        for z in range(4):
            for j in range(2):
                q = 4 * z + 2 * side + j
                high = q // 8
                places.append(2 * ((y - q % 8 + 8) % 8) + jnp.where(high == zh, 0, 1))
                groups.append(2 * z + side)
    n_q = len(places)
    step = 1 - 2 * core
    firsts = [n_own * core, n_own * (1 - core)]
    chunks = [(x, [own[pl.ds(f, n_own)] for f in firsts])]
    chunks.append((x - step, [near[pl.ds(f, n_own)] for f in firsts]))
    chunks.append((x + step, [near_other[pl.ds(f, n_own)] for f in firsts]))
    chunks.append((x + 2, [far[...], far_other[...]]))
    out = None
    for place, taus in chunks:
        at = pl.multiple_of(((place + 4) % 4) * width, 128)
        lhs = jnp.concatenate([ket[q, :, pl.ds(at, width)] for q in places], axis=0)
        rhs = jnp.concatenate(taus, axis=0).reshape(2 * n_own * rows, width)
        term = lax.dot_general(lhs, rhs, (((1,), (1,)), ((), ())), preferred_element_type=F32)
        out = term if out is None else out + term
    for side in range(2):
        for k in range(n_own):
            p = firsts[side] + k
            at = (side * n_own + k) * rows
            for i in range(n_q):
                wanted = lists[groups[i], 0] == p
                for m in range(1, lists.shape[1]):
                    wanted = jnp.logical_or(wanted, lists[groups[i], m] == p)
                block = out[i * cols : (i + 1) * cols, at : at + rows]
                block = jnp.where(wanted, block, 0.0).astype(BF16)
                half[pl.ds(pl.multiple_of(p * cols, 16), cols), i * rows : (i + 1) * rows] = block


def total_kernel(half, mine, theirs, out):
    parts, places, blocks, rows, width = mine.shape
    m = half.shape[0]
    keep = m * rows // 128
    n_c = places * blocks * rows
    for x in range(parts):
        sums = 0.0
        for side, ref in enumerate((mine, theirs)):
            rhs = ref[x].reshape(n_c, width)
            sums = sums + jnp.dot(half[:, side * n_c : (side + 1) * n_c], rhs, preferred_element_type=F32)
        for i in range(width // rows):
            block = sums[:, i * rows : (i + 1) * rows]
            tail = jnp.concatenate([block[keep:, 32 * s : 32 * s + 32] for s in range(rows // 32)], axis=0)
            out[x * (width // rows) + i] = jnp.concatenate([block[:keep], tail], axis=1).astype(BF16)


def sum_kernel(parts, out):
    rows = out.shape[1]
    keep, step = parts.shape[1], out.shape[0] - parts.shape[1]
    sums = parts[0].astype(F32)
    for i in range(1, parts.shape[0]):
        sums = sums + parts[i].astype(F32)
    out[:keep, :] = sums[:, :rows]
    tail = [sums[step * s : step * (s + 1), rows:] for s in range(rows // 32)]
    out[keep:, :] = jnp.concatenate(tail, axis=1)


def per_device(amplitudes, bra_factor, ket_factor, pair_list):
    pairs, rows, _ = amplitudes.shape
    cols = ket_factor.shape[1]
    n_a = bra_factor.shape[2]
    core = lax.axis_index("core")
    where = jnp.stack([lax.axis_index(name) for name in AXES]).astype(jnp.int32)
    n_own = n_a // lax.axis_size("x")

    ket = jnp.concatenate([ket_factor, shifted(ket_factor, "zh", 1)], axis=0)
    ahead, behind = [ket], [ket]
    for s in range(1, 5):
        ahead.append(shifted(ahead[-1], "y", 1))
        if s < 4:
            behind.append(shifted(behind[-1], "y", -1))
    kets = ahead + behind[:0:-1]
    own = lax.dynamic_slice_in_dim(bra_factor, n_own * lax.axis_index("x"), n_own, 2)
    bra = copies_from(copies_from(own, "zl"), "x")
    near = both_ways(amplitudes)
    far = lax.dynamic_slice_in_dim(amplitudes, core * (pairs // 2), pairs // 2, 0)
    far = shifted(far, "x", 2)
    taus = [amplitudes, near, shifted(near, "core", 1), far, shifted(far, "core", 1)]
    bra_other = shifted(bra, "core", 1)

    n_q = 2 * bra.shape[1] * bra.shape[2]
    half = pl.pallas_call(
        half_kernel,
        in_specs=[SMEM, SMEM] + [VMEM] * (len(kets) + len(taus)),
        out_specs=VMEM,
        out_shape=jax.ShapeDtypeStruct((pairs * cols, n_q * rows), BF16),
        scratch_shapes=[pltpu.VMEM((n_q, cols, ket.shape[2]), BF16)],
        compiler_params=PARAMS,
        name="half",
    )(pair_list, where, *kets, *taus)
    n_va = n_a // rows
    total = pl.pallas_call(
        total_kernel,
        in_specs=[VMEM] * 3,
        out_specs=VMEM,
        out_shape=jax.ShapeDtypeStruct((n_va, pairs * cols * rows // 128, 128), BF16),
        compiler_params=PARAMS,
        name="total",
    )(half, bra, bra_other)
    total = lax.all_to_all(total, VA, 0, 0, tiled=True)
    out = pl.pallas_call(
        sum_kernel,
        in_specs=[VMEM],
        out_specs=VMEM,
        out_shape=jax.ShapeDtypeStruct((pairs * cols, rows), F32),
        compiler_params=PARAMS,
        name="sum",
    )(total)
    return out.reshape(pairs, cols, rows).transpose(0, 2, 1)


def solution(mesh):
    torus = Mesh(mesh.devices.reshape(2, 8, 4, 2, 4), AXES)
    return jax.shard_map(
        per_device,
        mesh=torus,
        in_specs=(P(None, VA, "x"), P(("zl", "core"), VA, None), P(VA, ("zl", "core", "x"), None), P()),
        out_specs=P(None, VA, ("zl", "core", "x")),
        check_vma=False,
    )
```

```python
import functools

import jax
import jax.numpy as jnp
from jax import lax
from jax.experimental import pallas as pl
from jax.experimental.pallas import tpu as pltpu
from jax.sharding import Mesh
from jax.sharding import PartitionSpec as P

AXES = ("zh", "y", "zl", "core", "x")
VA = ("zh", "y")
F32 = jnp.float32
BF16 = jnp.bfloat16
VMEM = pl.BlockSpec(memory_space=pltpu.VMEM)
SMEM = pl.BlockSpec(memory_space=pltpu.SMEM)
PARAMS = pltpu.CompilerParams(vmem_limit_bytes=16 << 20)


def shifted(block, axis, by):
    n = lax.axis_size(axis)
    return lax.ppermute(block, axis, [(i, (i + by) % n) for i in range(n)])


def both_ways(block):
    n = lax.axis_size("x")
    route = [(n * c + i, n * c + (i + 1 - 2 * c) % n) for i in range(n) for c in range(2)]
    return lax.ppermute(block, ("core", "x"), route)


def copies_from(array, axis):
    copies = jnp.broadcast_to(array, (lax.axis_size(axis), *array.shape))
    return lax.all_to_all(copies, axis, 0, 0, tiled=True)


def position(name):
    return lax.axis_index(name).astype(jnp.int32)


def half_kernel(steps, lists, *refs):
    kets, refs = refs[: len(steps)], refs[len(steps) :]
    own, near, near_other, far, far_other = refs[:5]
    half = refs[-1]
    zh, y, _, core, x = [position(name) for name in AXES]
    n_own, rows, width = far.shape
    cols = kets[0].shape[1]
    step = 1 - 2 * core
    firsts = [n_own * core, n_own * (1 - core)]
    chunks = [(x, [own[pl.ds(f, n_own)] for f in firsts])]
    chunks.append((x - step, [near[pl.ds(f, n_own)] for f in firsts]))
    chunks.append((x + step, [near_other[pl.ds(f, n_own)] for f in firsts]))
    chunks.append((x + 2, [far[...], far_other[...]]))
    out = None
    for place, taus in chunks:
        at = pl.multiple_of(((place + 4) % 4) * width, 128)
        lhs = jnp.concatenate([ket[h, :, pl.ds(at, width)] for ket in kets for h in range(2)], axis=0)
        rhs = jnp.concatenate(taus, axis=0).reshape(2 * n_own * rows, width)
        term = lax.dot_general(lhs, rhs, (((1,), (1,)), ((), ())), preferred_element_type=F32)
        out = term if out is None else out + term
    if len(refs) > 6:
        for d in set(range(8)) - set(steps):
            half[2 * d : 2 * d + 2] = refs[5][2 * d : 2 * d + 2]
    for n, d in enumerate(steps):
        for h in range(2):
            high = zh if h == 0 else 1 - zh
            group = (8 * high + (y - d + 8) % 8) // 2
            i = 2 * n + h
            for side in range(2):
                for k in range(n_own):
                    p = firsts[side] + k
                    at = (side * n_own + k) * rows
                    wanted = lists[0, group] == p
                    for m in range(1, lists.shape[0]):
                        wanted = jnp.logical_or(wanted, lists[m, group] == p)
                    block = out[i * cols : (i + 1) * cols, at : at + rows]
                    block = jnp.where(wanted, block, 0.0).astype(BF16)
                    half[2 * d + h, pl.ds(pl.multiple_of(p * cols, 16), cols), :] = block


def half_of(steps, lists, kets, taus, before):
    pairs, rows, _ = taus[0].shape
    _, cols, _ = kets[0].shape
    earlier = [] if before is None else [before]
    operands = [kets[d] for d in steps] + taus + earlier
    return pl.pallas_call(
        functools.partial(half_kernel, steps),
        in_specs=[SMEM] + [VMEM] * len(operands),
        out_specs=VMEM,
        out_shape=jax.ShapeDtypeStruct((2 * len(kets), pairs * cols, rows), BF16),
        compiler_params=PARAMS,
    )(lists, *operands)


def total_kernel(half, mine, theirs, out, lhs):
    parts, places, blocks, rows, width = mine.shape
    zh, y, _, core, _ = [position(name) for name in AXES]
    m = half.shape[1]
    keep = m * rows // 128
    n = 0
    for r in range(2):
        side = core if r == 0 else 1 - core
        for z in range(places):
            for j in range(blocks):
                q = places * z + blocks * side + j
                slot = 2 * ((y - q % 8 + 8) % 8) + jnp.where(q // 8 == zh, 0, 1)
                lhs[:, n : n + rows] = half[slot]
                n += rows
    n_c = places * blocks * rows
    for x in range(parts):
        sums = 0.0
        for side, ref in enumerate((mine, theirs)):
            rhs = ref[x].reshape(n_c, width)
            sums = sums + jnp.dot(lhs[:, side * n_c : (side + 1) * n_c], rhs, preferred_element_type=F32)
        for i in range(width // rows):
            block = sums[:, i * rows : (i + 1) * rows]
            tail = jnp.concatenate([block[keep:, 32 * s : 32 * s + 32] for s in range(rows // 32)], axis=0)
            va = x * (width // rows) + i
            out[va % 8 * 2 + va // 8] = jnp.concatenate([block[:keep], tail], axis=1).astype(BF16)


def sum_kernel(parts, out):
    rows = out.shape[1]
    keep, step = parts.shape[1], out.shape[0] - parts.shape[1]
    sums = parts[0].astype(F32)
    for i in range(1, parts.shape[0]):
        sums = sums + parts[i].astype(F32)
    out[:keep, :] = sums[:, :rows]
    tail = [sums[step * s : step * (s + 1), rows:] for s in range(rows // 32)]
    out[keep:, :] = jnp.concatenate(tail, axis=1)


def per_device(amplitudes, bra_factor, ket_factor, pair_list):
    pairs, rows, _ = amplitudes.shape
    cols = ket_factor.shape[1]
    n_a = bra_factor.shape[2]
    core = lax.axis_index("core")
    n_own = n_a // lax.axis_size("x")

    ket = jnp.concatenate([ket_factor, shifted(ket_factor, "zh", 1)], axis=0)
    ahead, behind = [ket], [ket]
    for s in range(1, 5):
        ahead.append(shifted(ahead[-1], "y", 1))
        if s < 4:
            behind.append(shifted(behind[-1], "y", -1))
    kets = ahead + behind[:0:-1]
    own = lax.dynamic_slice_in_dim(bra_factor, n_own * lax.axis_index("x"), n_own, 2)
    bra = copies_from(copies_from(own, "zl"), "x")
    near = both_ways(amplitudes)
    far = lax.dynamic_slice_in_dim(amplitudes, core * (pairs // 2), pairs // 2, 0)
    far = shifted(far, "x", 2)
    taus = [amplitudes, near, shifted(near, "core", 1), far, shifted(far, "core", 1)]
    bra_other = shifted(bra, "core", 1)

    half = half_of((0, 1, 2, 6, 7), pair_list.T, kets, taus, None)
    half = half_of((3, 4, 5), pair_list.T, kets, taus, half)
    n_va = n_a // rows
    total = pl.pallas_call(
        total_kernel,
        in_specs=[VMEM] * 3,
        out_specs=VMEM,
        out_shape=jax.ShapeDtypeStruct((n_va, pairs * cols * rows // 128, 128), BF16),
        scratch_shapes=[pltpu.VMEM((pairs * cols, half.shape[0] * rows), BF16)],
        compiler_params=PARAMS,
        name="total",
    )(half, bra, bra_other)
    total = lax.all_to_all(total, ("y", "zh"), 0, 0, tiled=True)
    out = pl.pallas_call(
        sum_kernel,
        in_specs=[VMEM],
        out_specs=VMEM,
        out_shape=jax.ShapeDtypeStruct((pairs * cols, rows), F32),
        compiler_params=PARAMS,
        name="sum",
    )(total)
    return out.reshape(pairs, cols, rows).transpose(0, 2, 1)


def solution(mesh):
    torus = Mesh(mesh.devices.reshape(2, 8, 4, 2, 4), AXES)
    return jax.shard_map(
        per_device,
        mesh=torus,
        in_specs=(P(None, VA, "x"), P(("zl", "core"), VA, None), P(VA, ("zl", "core", "x"), None), P()),
        out_specs=P(None, VA, ("zl", "core", "x")),
        check_vma=False,
    )
```

```python
import functools

import jax
import jax.numpy as jnp
from jax import lax
from jax.experimental import pallas as pl
from jax.experimental.pallas import tpu as pltpu
from jax.sharding import Mesh
from jax.sharding import PartitionSpec as P

AXES = ("zh", "y", "zl", "core", "x")
VA = ("zh", "y")
F32 = jnp.float32
BF16 = jnp.bfloat16
VMEM = pl.BlockSpec(memory_space=pltpu.VMEM)
SMEM = pl.BlockSpec(memory_space=pltpu.SMEM)
PARAMS = pltpu.CompilerParams(vmem_limit_bytes=16 << 20)


def shifted(block, axis, by):
    n = lax.axis_size(axis)
    return lax.ppermute(block, axis, [(i, (i + by) % n) for i in range(n)])


def both_ways(block):
    n = lax.axis_size("x")
    route = [(n * c + i, n * c + (i + 1 - 2 * c) % n) for i in range(n) for c in range(2)]
    return lax.ppermute(block, ("core", "x"), route)


def copies_from(array, axis):
    copies = jnp.broadcast_to(array, (lax.axis_size(axis), *array.shape))
    return lax.all_to_all(copies, axis, 0, 0, tiled=True)


def position(name):
    return lax.axis_index(name).astype(jnp.int32)


def half_kernel(steps, lists, *refs):
    kets, refs = refs[: len(steps)], refs[len(steps) :]
    own, near, near_other, far, far_other = refs[:5]
    half = refs[-1]
    zh, y, _, core, x = [position(name) for name in AXES]
    n_own, rows, width = far.shape
    cols = kets[0].shape[1]
    step = 1 - 2 * core
    firsts = [n_own * core, n_own * (1 - core)]
    chunks = [(x, [own[pl.ds(f, n_own)] for f in firsts])]
    chunks.append((x - step, [near[pl.ds(f, n_own)] for f in firsts]))
    chunks.append((x + step, [near_other[pl.ds(f, n_own)] for f in firsts]))
    chunks.append((x + 2, [far[...], far_other[...]]))
    out = None
    for place, taus in chunks:
        at = pl.multiple_of(((place + 4) % 4) * width, 128)
        lhs = jnp.concatenate([ket[h, :, pl.ds(at, width)] for ket in kets for h in range(2)], axis=0)
        rhs = jnp.concatenate(taus, axis=0).reshape(2 * n_own * rows, width)
        term = lax.dot_general(lhs, rhs, (((1,), (1,)), ((), ())), preferred_element_type=F32)
        out = term if out is None else out + term
    if len(refs) > 6:
        for d in set(range(8)) - set(steps):
            half[2 * d : 2 * d + 2] = refs[5][2 * d : 2 * d + 2]
    for n, d in enumerate(steps):
        for h in range(2):
            high = zh if h == 0 else 1 - zh
            group = (8 * high + (y - d + 8) % 8) // 2
            i = 2 * n + h
            for side in range(2):
                for k in range(n_own):
                    p = firsts[side] + k
                    at = (side * n_own + k) * rows
                    wanted = lists[0, group] == p
                    for m in range(1, lists.shape[0]):
                        wanted = jnp.logical_or(wanted, lists[m, group] == p)
                    block = out[i * cols : (i + 1) * cols, at : at + rows]
                    block = jnp.where(wanted, block, 0.0).astype(BF16)
                    half[2 * d + h, pl.ds(pl.multiple_of(p * cols, 16), cols), :] = block


def half_of(steps, lists, kets, taus, before):
    pairs, rows, _ = taus[0].shape
    _, cols, _ = kets[0].shape
    earlier = [] if before is None else [before]
    operands = [kets[d] for d in steps] + taus + earlier
    return pl.pallas_call(
        functools.partial(half_kernel, steps),
        in_specs=[SMEM] + [VMEM] * len(operands),
        out_specs=VMEM,
        out_shape=jax.ShapeDtypeStruct((2 * len(kets), pairs * cols, rows), BF16),
        compiler_params=PARAMS,
    )(lists, *operands)


def total_kernel(half, mine, theirs, out, lhs):
    parts, places, blocks, rows, width = mine.shape
    zh, y, _, core, _ = [position(name) for name in AXES]
    m = half.shape[1]
    keep = m * rows // 128
    n = 0
    for r in range(2):
        side = core if r == 0 else 1 - core
        for z in range(places):
            for j in range(blocks):
                q = places * z + blocks * side + j
                slot = 2 * ((y - q % 8 + 8) % 8) + jnp.where(q // 8 == zh, 0, 1)
                lhs[:, n : n + rows] = half[slot]
                n += rows
    n_c = places * blocks * rows
    for x in range(parts):
        sums = 0.0
        for side, ref in enumerate((mine, theirs)):
            rhs = ref[x].reshape(n_c, width)
            sums = sums + jnp.dot(lhs[:, side * n_c : (side + 1) * n_c], rhs, preferred_element_type=F32)
        for i in range(width // rows):
            block = sums[:, i * rows : (i + 1) * rows]
            tail = jnp.concatenate([block[keep:, 32 * s : 32 * s + 32] for s in range(rows // 32)], axis=0)
            out[x * (width // rows) + i] = jnp.concatenate([block[:keep], tail], axis=1).astype(BF16)


def sum_kernel(parts, out):
    rows = out.shape[1]
    keep, step = parts.shape[1], out.shape[0] - parts.shape[1]
    sums = parts[0].astype(F32)
    for i in range(1, parts.shape[0]):
        sums = sums + parts[i].astype(F32)
    out[:keep, :] = sums[:, :rows]
    tail = [sums[step * s : step * (s + 1), rows:] for s in range(rows // 32)]
    out[keep:, :] = jnp.concatenate(tail, axis=1)


def per_device(amplitudes, bra_factor, ket_factor, pair_list):
    pairs, rows, _ = amplitudes.shape
    cols = ket_factor.shape[1]
    n_a = bra_factor.shape[2]
    core = lax.axis_index("core")
    n_own = n_a // lax.axis_size("x")

    ket = jnp.concatenate([ket_factor, shifted(ket_factor, "zh", 1)], axis=0)
    ahead, behind = [ket], [ket]
    for s in range(1, 5):
        ahead.append(shifted(ahead[-1], "y", 1))
        if s < 4:
            behind.append(shifted(behind[-1], "y", -1))
    kets = ahead + behind[:0:-1]
    own = lax.dynamic_slice_in_dim(bra_factor, n_own * lax.axis_index("x"), n_own, 2)
    bra = copies_from(copies_from(own, "zl"), "x")
    near = both_ways(amplitudes)
    far = lax.dynamic_slice_in_dim(amplitudes, core * (pairs // 2), pairs // 2, 0)
    far = shifted(far, "x", 2)
    taus = [amplitudes, near, shifted(near, "core", 1), far, shifted(far, "core", 1)]
    bra_other = shifted(bra, "core", 1)

    half = half_of((0, 1, 2, 6, 7), pair_list.T, kets, taus, None)
    half = half_of((3, 4, 5), pair_list.T, kets, taus, half)
    n_va = n_a // rows
    total = pl.pallas_call(
        total_kernel,
        in_specs=[VMEM] * 3,
        out_specs=VMEM,
        out_shape=jax.ShapeDtypeStruct((n_va, pairs * cols * rows // 128, 128), BF16),
        scratch_shapes=[pltpu.VMEM((pairs * cols, half.shape[0] * rows), BF16)],
        compiler_params=PARAMS,
        name="total",
    )(half, bra, bra_other)
    total = lax.all_to_all(total, VA, 0, 0, tiled=True)
    out = pl.pallas_call(
        sum_kernel,
        in_specs=[VMEM],
        out_specs=VMEM,
        out_shape=jax.ShapeDtypeStruct((pairs * cols, rows), F32),
        compiler_params=PARAMS,
        name="sum",
    )(total)
    return out.reshape(pairs, cols, rows).transpose(0, 2, 1)


def solution(mesh):
    torus = Mesh(mesh.devices.reshape(2, 8, 4, 2, 4), AXES)
    return jax.shard_map(
        per_device,
        mesh=torus,
        in_specs=(P(None, VA, "x"), P(("zl", "core"), VA, None), P(VA, ("zl", "core", "x"), None), P()),
        out_specs=P(None, VA, ("zl", "core", "x")),
        check_vma=False,
    )
```

```python
import functools

import jax
import jax.numpy as jnp
from jax import lax
from jax.experimental import pallas as pl
from jax.experimental.pallas import tpu as pltpu
from jax.sharding import Mesh
from jax.sharding import PartitionSpec as P

AXES = ("zh", "y", "zl", "core", "x")
VA = ("zh", "y")
F32 = jnp.float32
BF16 = jnp.bfloat16
VMEM = pl.BlockSpec(memory_space=pltpu.VMEM)
SMEM = pl.BlockSpec(memory_space=pltpu.SMEM)
PARAMS = pltpu.CompilerParams(vmem_limit_bytes=16 << 20)


def shifted(block, axis, by):
    n = lax.axis_size(axis)
    return lax.ppermute(block, axis, [(i, (i + by) % n) for i in range(n)])


def both_ways(block):
    n = lax.axis_size("x")
    route = [(n * c + i, n * c + (i + 1 - 2 * c) % n) for i in range(n) for c in range(2)]
    return lax.ppermute(block, ("core", "x"), route)


def copies_from(array, axis):
    copies = jnp.broadcast_to(array, (lax.axis_size(axis), *array.shape))
    return lax.all_to_all(copies, axis, 0, 0, tiled=True)


def position(name):
    return lax.axis_index(name).astype(jnp.int32)


def half_kernel(steps, lists, *refs):
    kets, refs = refs[: len(steps)], refs[len(steps) :]
    own, near, near_other, far = refs[:4]
    half = refs[-1]
    zh, y, _, core, x = [position(name) for name in AXES]
    pairs, rows, width = own.shape
    n_own = pairs // 2
    cols = kets[0].shape[1]
    step = 1 - 2 * core
    firsts = [n_own * core, n_own * (1 - core)]
    chunks = [(x, [own[pl.ds(f, n_own)] for f in firsts])]
    chunks.append((x - step, [near[pl.ds(f, n_own)] for f in firsts]))
    chunks.append((x + step, [near_other[pl.ds(f, n_own)] for f in firsts]))
    chunks.append((x + 2, [far[pl.ds(f, n_own)] for f in firsts]))
    out = None
    for place, taus in chunks:
        at = pl.multiple_of(((place + 4) % 4) * width, 128)
        lhs = jnp.concatenate([ket[h, :, pl.ds(at, width)] for ket in kets for h in range(2)], axis=0)
        rhs = jnp.concatenate(taus, axis=0).reshape(2 * n_own * rows, width)
        term = lax.dot_general(lhs, rhs, (((1,), (1,)), ((), ())), preferred_element_type=F32)
        out = term if out is None else out + term
    if len(refs) > 5:
        for d in set(range(8)) - set(steps):
            half[2 * d : 2 * d + 2] = refs[4][2 * d : 2 * d + 2]
    for n, d in enumerate(steps):
        for h in range(2):
            high = zh if h == 0 else 1 - zh
            group = (8 * high + (y - d + 8) % 8) // 2
            i = 2 * n + h
            for side in range(2):
                for k in range(n_own):
                    p = firsts[side] + k
                    at = (side * n_own + k) * rows
                    wanted = lists[0, group] == p
                    for m in range(1, lists.shape[0]):
                        wanted = jnp.logical_or(wanted, lists[m, group] == p)
                    block = out[i * cols : (i + 1) * cols, at : at + rows]
                    block = jnp.where(wanted, block, 0.0).astype(BF16)
                    half[2 * d + h, pl.ds(pl.multiple_of(p * cols, 16), cols), :] = block


def half_of(steps, lists, kets, taus, before):
    pairs, rows, _ = taus[0].shape
    _, cols, _ = kets[0].shape
    earlier = [] if before is None else [before]
    operands = [kets[d] for d in steps] + taus + earlier
    return pl.pallas_call(
        functools.partial(half_kernel, steps),
        in_specs=[SMEM] + [VMEM] * len(operands),
        out_specs=VMEM,
        out_shape=jax.ShapeDtypeStruct((2 * len(kets), pairs * cols, rows), BF16),
        compiler_params=PARAMS,
    )(lists, *operands)


def total_kernel(half, mine, theirs, out, lhs):
    parts, places, blocks, rows, width = mine.shape
    zh, y, _, core, _ = [position(name) for name in AXES]
    m = half.shape[1]
    keep = m * rows // 128
    n = 0
    for r in range(2):
        side = core if r == 0 else 1 - core
        for z in range(places):
            for j in range(blocks):
                q = places * z + blocks * side + j
                slot = 2 * ((y - q % 8 + 8) % 8) + jnp.where(q // 8 == zh, 0, 1)
                lhs[:, n : n + rows] = half[slot]
                n += rows
    n_c = places * blocks * rows
    for x in range(parts):
        sums = 0.0
        for side, ref in enumerate((mine, theirs)):
            rhs = ref[x].reshape(n_c, width)
            sums = sums + jnp.dot(lhs[:, side * n_c : (side + 1) * n_c], rhs, preferred_element_type=F32)
        for i in range(width // rows):
            block = sums[:, i * rows : (i + 1) * rows]
            tail = jnp.concatenate([block[keep:, 32 * s : 32 * s + 32] for s in range(rows // 32)], axis=0)
            out[x * (width // rows) + i] = jnp.concatenate([block[:keep], tail], axis=1).astype(BF16)


def sum_kernel(parts, out):
    rows = out.shape[1]
    keep, step = parts.shape[1], out.shape[0] - parts.shape[1]
    sums = parts[0].astype(F32)
    for i in range(1, parts.shape[0]):
        sums = sums + parts[i].astype(F32)
    out[:keep, :] = sums[:, :rows]
    tail = [sums[step * s : step * (s + 1), rows:] for s in range(rows // 32)]
    out[keep:, :] = jnp.concatenate(tail, axis=1)


def per_device(amplitudes, bra_factor, ket_factor, pair_list):
    pairs, rows, _ = amplitudes.shape
    cols = ket_factor.shape[1]
    n_a = bra_factor.shape[2]
    n_own = n_a // lax.axis_size("x")

    ket = jnp.concatenate([ket_factor, shifted(ket_factor, "zh", 1)], axis=0)
    ahead, behind = [ket], [ket]
    for s in range(1, 5):
        ahead.append(shifted(ahead[-1], "y", 1))
        if s < 4:
            behind.append(shifted(behind[-1], "y", -1))
    kets = ahead + behind[:0:-1]
    own = lax.dynamic_slice_in_dim(bra_factor, n_own * lax.axis_index("x"), n_own, 2)
    bra = copies_from(copies_from(own, "zl"), "x")
    near = both_ways(amplitudes)
    far = both_ways(near)
    taus = [amplitudes, near, shifted(near, "core", 1), far]
    bra_other = shifted(bra, "core", 1)

    half = half_of((0, 1, 2, 6, 7), pair_list.T, kets, taus, None)
    half = half_of((3, 4, 5), pair_list.T, kets, taus, half)
    n_va = n_a // rows
    total = pl.pallas_call(
        total_kernel,
        in_specs=[VMEM] * 3,
        out_specs=VMEM,
        out_shape=jax.ShapeDtypeStruct((n_va, pairs * cols * rows // 128, 128), BF16),
        scratch_shapes=[pltpu.VMEM((pairs * cols, half.shape[0] * rows), BF16)],
        compiler_params=PARAMS,
        name="total",
    )(half, bra, bra_other)
    total = lax.all_to_all(total, VA, 0, 0, tiled=True)
    out = pl.pallas_call(
        sum_kernel,
        in_specs=[VMEM],
        out_specs=VMEM,
        out_shape=jax.ShapeDtypeStruct((pairs * cols, rows), F32),
        compiler_params=PARAMS,
        name="sum",
    )(total)
    return out.reshape(pairs, cols, rows).transpose(0, 2, 1)


def solution(mesh):
    torus = Mesh(mesh.devices.reshape(2, 8, 4, 2, 4), AXES)
    return jax.shard_map(
        per_device,
        mesh=torus,
        in_specs=(P(None, VA, "x"), P(("zl", "core"), VA, None), P(VA, ("zl", "core", "x"), None), P()),
        out_specs=P(None, VA, ("zl", "core", "x")),
        check_vma=False,
    )
```
